32 devices in a mesh: spin: 1 (over z), row: 4 (over y), col: 8 (over x, core).
Axes of the slice: x: 4, y: 4, z: 1, core: 2. Of those that a mesh axis runs over, the one named last changes fastest.
The devices are a block of a 4x4x8 slice.
Arguments:
- hamiltonian: float32 [3072, 3072], P(('spin', 'row'), 'col')
- bounds: float32 [2], P('spin')
- n_occ: int32 [1], P('spin')
Outputs:
- output 1: float32 [3072, 3072], P(('spin', 'row'), 'col')
- output 2: float32 [1], P('spin')
All inputs are finite; a program needn't handle non-finite values.
Results may differ from the reference program's by a relative error of at most 0.001.
Values sent between devices are 32-bit elements.
A program may use at most 768 MiB of HBM per device.

```python
import jax
import jax.numpy as jnp
from jax import lax

N = 3072
STEPS = 3


def setup_inputs(seed: int = 0, part: int = 0) -> dict:
    key = jax.random.fold_in(jax.random.key(seed), part)
    k_off, k_diag, k_shift, k_margin, k_occ = jax.random.split(key, 5)
    gauss_mat = jax.random.normal(k_off, (N, N), jnp.float32)
    sym_part = (gauss_mat + gauss_mat.T) * (2.0 * N) ** -0.5
    unif_diag = jax.random.uniform(k_diag, (N,), jnp.float32)
    shift_val = 2.0 + jax.random.uniform(k_shift, (), jnp.float32)
    diag_vals = shift_val + 0.8 * (3.0 * unif_diag * unif_diag - 1.0)
    index_vec = jnp.arange(N)
    on_diag = index_vec[:, None] == index_vec[None, :]
    hamiltonian = jnp.where(on_diag, diag_vals[None, :], sym_part)
    margins = jax.random.uniform(k_margin, (2,), jnp.float32, 0.0, 0.5)
    bounds = jnp.stack([jnp.min(diag_vals) - 2.4 - margins[0], jnp.max(diag_vals) + 2.4 + margins[1]])
    n_occ = jax.random.randint(k_occ, (1,), 3 * N // 20, 7 * N // 20 + 1, jnp.int32)
    return {"hamiltonian": hamiltonian, "bounds": bounds, "n_occ": n_occ}


def reference(hamiltonian, bounds, n_occ):
    occupied = n_occ[0].astype(jnp.float32)
    mu_val = jnp.trace(hamiltonian) / N
    lam_scale = jnp.minimum(occupied / (bounds[1] - mu_val), (N - occupied) / (mu_val - bounds[0]))
    identity = jnp.eye(N, dtype=jnp.float32)
    density = (lam_scale / N) * (mu_val * identity - hamiltonian) + (occupied / N) * identity

    def purify_step(dens_cur, unused_x):
        dens_sq = jnp.dot(dens_cur, dens_cur, preferred_element_type=jnp.float32, precision=lax.Precision.HIGHEST)
        dens_cube = jnp.dot(dens_sq, dens_cur, preferred_element_type=jnp.float32, precision=lax.Precision.HIGHEST)
        trace_x = jnp.trace(dens_cur)
        trace_sq = jnp.sum(dens_cur * dens_cur)
        trace_cube = jnp.sum(dens_sq * dens_cur)
        mix_coef = (trace_sq - trace_cube) / (trace_x - trace_sq)
        updated = ((1.0 - 2.0 * mix_coef) * dens_cur + (1.0 + mix_coef) * dens_sq - dens_cube) / (1.0 - mix_coef)
        return updated, None

    density, _ = lax.scan(purify_step, density, None, length=STEPS)
    energy = 2.0 * jnp.sum(density * hamiltonian)
    return density, energy[None]
```

```python
import functools

import jax
import jax.numpy as jnp
from jax import lax
from jax.experimental import pallas as pl
from jax.experimental.pallas import tpu as pltpu
from jax.sharding import PartitionSpec as P

STEPS = 3
RING = 4
CORES = 2
PARTS = 3
PIECES = 12
MESH = pl.DeviceIdType.MESH
HIGHEST = lax.Precision.HIGHEST


def purify(
    ham, bounds, n_occ, out, energy,
    cols, rows, sq, acc, tin, ham_t, red_a, red_b,
    x_recv, xf_recv, y_recv, yf_recv, d_recv, x_send, xf_send, y_send, yf_send, d_send,
    x2_recv, d2_recv, t_recv, x2_send, d2_send, t_send, a_recv, a_send, b_recv, b_send,
):
    cb, rb = ham.shape
    qr = rb // PARTS
    hr = qr // 2
    pr = rb // PIECES
    order = cb * RING
    per = PIECES // PARTS
    i = lax.axis_index("row")
    jc = lax.axis_index("col")
    j = lax.div(jc, CORES)
    c = lax.rem(jc, CORES)
    n_col = RING * CORES

    def wrap(v):
        return lax.rem(v + RING, RING)

    p = wrap(j - i)
    diag_chip = p == 0
    left, right = wrap(j + 3), wrap(j + 1)
    up, down = wrap(i + 3), wrap(i + 1)
    opp, iopp = wrap(j + 2), wrap(i + 2)
    partner = {"col": j * CORES + (1 - c)}
    to_x = ({"col": right * CORES + c}, {"col": left * CORES + c})
    to_y = ({"row": down}, {"row": up})
    half_cols = pl.ds(pl.multiple_of(c * rb, rb), rb)

    def copy(src, dst, send, recv, dev):
        return pltpu.make_async_remote_copy(
            src_ref=src, dst_ref=dst, send_sem=send, recv_sem=recv, device_id=dev, device_id_type=MESH
        )

    def send(ref, ss, rs, dev):
        copy(ref, ref, ss, rs, dev).start()

    def wait_recv(ref, rs):
        copy(ref, ref, d_send.at[0], rs, partner).wait_recv()

    def wait_send(ref, ss):
        copy(ref, ref, ss, d_recv.at[0, 0], partner).wait_send()

    def red_put(idx, vals):
        sub = lax.broadcasted_iota(jnp.int32, (8, 128), 0)
        tile = jnp.zeros((8, 128), jnp.float32)
        for r, v in enumerate(vals):
            tile = jnp.where(sub == r, v, tile)
        red_a[idx, jc] = tile

    def red_send(idx):
        for k in range(1, n_col):
            dev = lax.rem(jc + k, n_col)
            send(red_a.at[idx, jc], a_send.at[idx], a_recv.at[idx], {"col": dev})

    def red_mid_put(idx):
        wait_recv(red_a.at[idx, pl.ds(0, n_col - 1)], a_recv.at[idx])
        red_b[idx, i] = jnp.sum(red_a[idx], axis=0)

    def red_mid_send(idx):
        for k in range(1, RING):
            send(red_b.at[idx, i], b_send.at[idx], b_recv.at[idx], {"row": wrap(i + k)})

    def red_get(idx):
        wait_recv(red_b.at[idx, pl.ds(0, RING - 1)], b_recv.at[idx])
        wait_send(red_a.at[idx, pl.ds(0, n_col - 1)], a_send.at[idx])
        wait_send(red_b.at[idx, pl.ds(0, RING - 1)], b_send.at[idx])
        total = jnp.sum(red_b[idx], axis=0)
        return [total[r : r + 1, 0:1] for r in range(3)]

    def total_of(v):
        return jnp.sum(v, axis=1, keepdims=True)

    def is_diag(m):
        row_id = lax.broadcasted_iota(jnp.int32, (pr, cb), 0) + (m * pr + c * rb + (j - i) * cb)
        return row_id == lax.broadcasted_iota(jnp.int32, (pr, cb), 1)

    def piece_rows(m):
        return pl.ds(pl.multiple_of(lax.rem(m, per) * pr, pr), pr)

    def put_x(m, val, buf):
        cols[j, lax.div(m, per), c, piece_rows(m)] = val
        for q in range(PARTS):
            for h in range(CORES):
                at = h * rb + q * qr
                rows[buf, i, q, h, pl.ds(pl.multiple_of(m * pr, pr), pr)] = val[:, at : at + qr]

    barrier = pltpu.get_barrier_semaphore()
    for k in range(1, n_col):
        pl.semaphore_signal(barrier, inc=1, device_id={"col": lax.rem(jc + k, n_col)}, device_id_type=MESH)
    for k in range(1, RING):
        pl.semaphore_signal(barrier, inc=1, device_id={"row": wrap(i + k)}, device_id_type=MESH)
    for t in range(cb // qr):
        ham_t[:, t * qr : (t + 1) * qr] = ham[t * qr : (t + 1) * qr, :].T

    def trace_body(m, tr):
        blk = ham_t[pl.ds(pl.multiple_of(m * pr, pr), pr)]
        return tr + jnp.sum(jnp.where(is_diag(m), blk, 0.0), axis=0, keepdims=True)

    tr = lax.fori_loop(0, PIECES, trace_body, jnp.zeros((1, cb), jnp.float32))
    red_put(0, [total_of(tr)])
    pl.semaphore_wait(barrier, n_col + RING - 2)
    red_send(0)
    red_mid_put(0)
    red_mid_send(0)
    mu = red_get(0)[0] / order
    occ = jnp.full((1, 1), n_occ[0].astype(jnp.float32))
    eps_min = jnp.full((1, 1), bounds[0])
    eps_max = jnp.full((1, 1), bounds[1])
    lam = jnp.minimum(occ / (eps_max - mu), (order - occ) / (mu - eps_min)) / order

    @pl.loop(0, PIECES)
    def _(m):
        blk = ham_t[pl.ds(pl.multiple_of(m * pr, pr), pr)]
        put_x(m, jnp.where(is_diag(m), lam * (mu - blk) + occ / order, -lam * blk), 0)

    def step(s, carry):
        buf = lax.rem(s, 2)

        for q in range(PARTS):
            for o in range(2):
                for d in range(2):
                    h = d if o == 0 else 1 - d
                    send(cols.at[j, q, c, pl.ds(h * hr, hr)], x_send.at[d], x_recv.at[d, q, h], to_x[d])
                    send(rows.at[buf, i, q, h], y_send.at[d], y_recv.at[d, q, h], to_y[d])
            send(cols.at[j, q, c], d_send.at[0], d_recv.at[0, q], partner)
        acc[...] = jnp.zeros_like(acc)

        near = ((left, up), (right, down))

        def arrive_near(q):
            for d in range(2):
                kx, ky = near[d]
                xp = cols.at[kx, q, c, pl.ds(d * hr, hr)]
                wait_recv(xp, x_recv.at[d, q, d])
                send(xp, xf_send.at[d], xf_recv.at[d, q], to_x[d])
                yp = rows.at[buf, ky, q, d]
                wait_recv(yp, y_recv.at[d, q, d])
                send(yp, yf_send.at[d], yf_recv.at[d, q], to_y[d])
            for d in range(2):
                kx, ky = near[d]
                wait_recv(cols.at[kx, q, c, pl.ds((1 - d) * hr, hr)], x_recv.at[d, q, 1 - d])
                send(cols.at[kx, q, c], d_send.at[0], d_recv.at[3 if d == 0 else 1, q], partner)
                wait_recv(rows.at[buf, ky, q, 1 - d], y_recv.at[d, q, 1 - d])

        def arrive_far(q):
            for d in range(2):
                wait_recv(cols.at[opp, q, c, pl.ds(d * hr, hr)], xf_recv.at[d, q])
            send(cols.at[opp, q, c], d_send.at[0], d_recv.at[2, q], partner)
            for d in range(2):
                wait_recv(rows.at[buf, iopp, q, d], yf_recv.at[d, q])

        def item1(t, carry):
            in1 = t < jnp.where(diag_chip, 9, 6)
            late = jnp.maximum(t - 6, 0)
            q = jnp.where(
                in1,
                jnp.where(diag_chip, lax.div(t, 3), lax.div(t, 2)),
                jnp.where(diag_chip, jnp.maximum(t - 9, 0), lax.div(late, 2)),
            )
            u = jnp.where(
                in1,
                jnp.where(diag_chip, lax.rem(t, 3), lax.rem(t, 2)),
                jnp.where(diag_chip, 0, lax.rem(late, 2)),
            )
            k1 = jnp.where(
                diag_chip,
                i + jnp.where(u == 2, 3, u),
                jnp.where(p == 2, i + jnp.where(u == 0, 1, 3), jnp.where(u == 0, j, i)),
            )
            k = wrap(jnp.where(in1, k1, jnp.where(u == 0, i + 2, j + 2)))

            @pl.when(jnp.logical_and(in1, u == 0))
            def _():
                arrive_near(q)

            @pl.when(jnp.logical_and(jnp.logical_not(in1), u == 0))
            def _():
                arrive_far(q)

            wait_recv(cols.at[k, q, 1 - c], d_recv.at[wrap(k - j), q])
            rhs = cols[k, q].reshape(CORES * qr, cb)
            own = cols[k, q, :, :, half_cols].reshape(CORES * qr, rb)
            lhs = jnp.concatenate(
                [jnp.concatenate([rows[buf, k, q, h] for h in range(CORES)], axis=1), own.T], axis=0
            )
            acc[...] += jnp.dot(lhs, rhs, precision=HIGHEST, preferred_element_type=jnp.float32)
            return carry

        lax.fori_loop(0, RING * PARTS, item1, 0)
        for d in range(2):
            wait_send(cols.at[j, :, c], x_send.at[d])
            wait_send(cols.at[j, :, c, pl.ds(0, hr)], xf_send.at[d])
            wait_send(rows.at[buf, i], y_send.at[d])
            wait_send(rows.at[buf, i, :, 0], yf_send.at[d])
        wait_send(cols.at[:, :, c], d_send.at[0])

        for q in range(PARTS):
            sq[j, q, c] = acc[q * qr : (q + 1) * qr]

        @pl.when(jnp.logical_not(diag_chip))
        def _():
            for q in range(PARTS):
                sq[i, q, c] = acc[rb + q * qr : rb + (q + 1) * qr]

        def sums_body(m, carry):
            x = cols[j, lax.div(m, per), c, piece_rows(m)]
            x2 = acc[pl.ds(pl.multiple_of(m * pr, pr), pr)]
            t1 = jnp.sum(jnp.where(is_diag(m), x, 0.0), axis=0, keepdims=True)
            t2 = jnp.sum(x * x, axis=0, keepdims=True)
            t3 = jnp.sum(x2 * x, axis=0, keepdims=True)
            return carry[0] + t1, carry[1] + t2, carry[2] + t3

        zero = jnp.zeros((1, cb), jnp.float32)
        sums = lax.fori_loop(0, PIECES, sums_body, (zero, zero, zero))
        red_put(s + 1, [total_of(v) for v in sums])

        k_left = jnp.where(p == 1, opp, left)
        k_right = jnp.where(p == 3, opp, right)

        @pl.when(jnp.logical_not(diag_chip))
        def _():
            for m in range(PIECES):
                for d in range(2):
                    ref = sq.at[j, m // per, c, pl.ds((m % per) * pr, pr)]
                    send(ref, x2_send.at[d], x2_recv.at[d, m], to_x[d])

        @pl.when(p == 2)
        def _():
            for q in range(PARTS):
                for h in range(CORES):
                    src = sq.at[j, :, c, :, pl.ds(h * rb + q * qr, qr)]
                    copy(src, tin.at[q, h], t_send.at[0], t_recv.at[q, h], {"row": j}).start()

        for q in range(PARTS):
            send(sq.at[j, q, c], d2_send.at[0], d2_recv.at[0, q], partner)

        @pl.when(jnp.logical_not(diag_chip))
        def _():
            for q in range(PARTS):
                send(sq.at[i, q, c], d2_send.at[0], d2_recv.at[3, q], partner)

        red_send(s + 1)
        acc[0:rb] = jnp.zeros((rb, cb), jnp.float32)

        def arrive2(m):
            q = lax.div(m, per)
            u = lax.rem(m, per)
            for d, k in ((0, k_left), (1, k_right)):
                ref = sq.at[k, q, c, piece_rows(m)]
                wait_recv(ref, x2_recv.at[d, m])

                @pl.when(diag_chip)
                def _():
                    send(ref, x2_send.at[d], x2_recv.at[d, m], to_x[d])

            @pl.when(u == per - 1)
            def _():
                send(sq.at[k_left, q, c], d2_send.at[0], d2_recv.at[1, q], partner)
                send(sq.at[k_right, q, c], d2_send.at[0], d2_recv.at[2, q], partner)

            @pl.when(jnp.logical_and(diag_chip, u == per - 2))
            def _():
                for h in range(CORES):
                    wait_recv(tin.at[q, h], t_recv.at[q, h])
                    sq[opp, q, h, :, half_cols] = tin[q, h].reshape(rb, qr).T

            @pl.when(jnp.logical_and(diag_chip, u == per - 1))
            def _():
                ref = sq.at[opp, q, :, :, half_cols]
                send(ref, d2_send.at[0], d2_recv.at[3, q], partner)

        def item2(m, carry):
            @pl.when(m < PIECES)
            def _():
                arrive2(m)

            @pl.when(m == 3)
            def _():
                red_mid_put(s + 1)

            @pl.when(m == 4)
            def _():
                red_mid_send(s + 1)

            u = lax.rem(m, 4)
            qq = jnp.maximum(lax.div(m, 4) - 1, 0)
            early = m < 4
            kind = jnp.where(early, jnp.where(m < 3, 0, 3), u + 1)
            q = jnp.where(
                early, jnp.where(m < 3, m, 0), jnp.where(jnp.logical_and(u == 2, jnp.logical_not(diag_chip)), qq + 1, qq)
            )
            k = jnp.where(
                kind == 0, j, jnp.where(kind == 1, k_left, jnp.where(kind == 2, k_right, jnp.where(diag_chip, opp, i)))
            )
            work = jnp.where(
                early,
                jnp.logical_or(m < 3, jnp.logical_not(diag_chip)),
                jnp.logical_or(u < 2, jnp.logical_and(u == 2, jnp.logical_or(diag_chip, qq < 2))),
            )

            @pl.when(work)
            def _():
                @pl.when(jnp.logical_and(kind == 3, diag_chip))
                def _():
                    other = pl.ds(pl.multiple_of((1 - c) * rb, rb), rb)
                    wait_recv(sq.at[k, q, :, :, other], d2_recv.at[3, q])

                @pl.when(jnp.logical_not(jnp.logical_and(kind == 3, diag_chip)))
                def _():
                    wait_recv(sq.at[k, q, 1 - c], d2_recv.at[kind, q])

                lhs = jnp.concatenate([rows[buf, k, q, h] for h in range(CORES)], axis=1)
                rhs = sq[k, q].reshape(CORES * qr, cb)
                acc[0:rb] += jnp.dot(lhs, rhs, precision=HIGHEST, preferred_element_type=jnp.float32)

            return carry

        lax.fori_loop(0, PIECES + 3, item2, 0)
        for d in range(2):
            wait_send(sq.at[j, :, c], x2_send.at[d])
        wait_send(sq.at[:, :, c], d2_send.at[0])

        @pl.when(p == 2)
        def _():
            wait_send(sq.at[j, :, c], t_send.at[0])

        t1, t2, t3 = red_get(s + 1)
        mix = (t2 - t3) / (t1 - t2)
        a1 = (1.0 - 2.0 * mix) / (1.0 - mix)
        a2 = (1.0 + mix) / (1.0 - mix)
        a3 = 1.0 / (1.0 - mix)

        def update_body(m, carry):
            at = pl.ds(pl.multiple_of(m * pr, pr), pr)
            x = cols[j, lax.div(m, per), c, piece_rows(m)]
            x2 = sq[j, lax.div(m, per), c, piece_rows(m)]
            new = a1 * x + a2 * x2 - a3 * acc[at]
            put_x(m, new, lax.rem(s + 1, 2))
            return carry + jnp.sum(new * ham_t[at], axis=0, keepdims=True)

        en = lax.fori_loop(0, PIECES, update_body, zero)
        return total_of(en)

    en = lax.fori_loop(0, STEPS, step, jnp.zeros((1, 1), jnp.float32))
    last = STEPS + 1
    red_put(last, [en])
    for q in range(PARTS):
        out[:, q * qr : (q + 1) * qr] = cols[j, q, c].T
    red_send(last)
    red_mid_put(last)
    red_mid_send(last)
    energy[0] = jnp.sum(2.0 * red_get(last)[0])


def solution(mesh):
    def local_fn(ham_blk, bounds, n_occ):
        cb, rb = ham_blk.shape
        qr = rb // PARTS
        f32 = jnp.float32
        dma = pltpu.SemaphoreType.DMA
        vmem = pl.BlockSpec(memory_space=pltpu.VMEM)
        smem = pl.BlockSpec(memory_space=pltpu.SMEM)
        return pl.pallas_call(
            purify,
            out_shape=(jax.ShapeDtypeStruct((cb, rb), f32), jax.ShapeDtypeStruct((1,), f32)),
            in_specs=[vmem, smem, smem],
            out_specs=(vmem, smem),
            scratch_shapes=[
                pltpu.VMEM((RING, PARTS, CORES, qr, cb), f32),
                pltpu.VMEM((2, RING, PARTS, CORES, rb, qr), f32),
                pltpu.VMEM((RING, PARTS, CORES, qr, cb), f32),
                pltpu.VMEM((cb, cb), f32),
                pltpu.VMEM((PARTS, CORES, PARTS, qr, qr), f32),
                pltpu.VMEM((rb, cb), f32),
                pltpu.VMEM((STEPS + 2, RING * CORES, 8, 128), f32),
                pltpu.VMEM((STEPS + 2, RING, 8, 128), f32),
                dma((2, PARTS, 2)), dma((2, PARTS)), dma((2, PARTS, 2)), dma((2, PARTS)), dma((RING, PARTS)),
                dma((2,)), dma((2,)), dma((2,)), dma((2,)), dma((1,)),
                dma((2, PIECES)), dma((4, PARTS)), dma((PARTS, CORES)), dma((2,)), dma((1,)), dma((1,)),
                dma((STEPS + 2,)), dma((STEPS + 2,)), dma((STEPS + 2,)), dma((STEPS + 2,)),
            ],
            compiler_params=pltpu.CompilerParams(
                collective_id=0, has_side_effects=True, vmem_limit_bytes=56 * 2**20
            ),
        )(ham_blk, bounds, n_occ)

    spec_mat = P(("spin", "row"), "col")
    return jax.shard_map(
        local_fn, mesh=mesh, in_specs=(spec_mat, P("spin"), P("spin")), out_specs=(spec_mat, P("spin")), check_vma=False
    )
```

```python
import functools

import jax
import jax.numpy as jnp
from jax import lax
from jax.experimental import pallas as pl
from jax.experimental.pallas import tpu as pltpu
from jax.sharding import PartitionSpec as P

STEPS = 3
RING = 4
CORES = 2
PARTS = 3
PIECES = 12
MESH = pl.DeviceIdType.MESH
HIGHEST = lax.Precision.HIGHEST


def purify(
    ham, bounds, n_occ, out, energy,
    cols, rows, sq, acc, tin, ham_t, red_a, red_b,
    x_recv, xf_recv, y_recv, yf_recv, d_recv, x_send, xf_send, y_send, yf_send, d_send,
    x2_recv, d2_recv, t_recv, x2_send, d2_send, t_send, a_recv, a_send, b_recv, b_send,
):
    cb, rb = ham.shape
    qr = rb // PARTS
    hr = qr // 2
    pr = rb // PIECES
    order = cb * RING
    per = PIECES // PARTS
    i = lax.axis_index("row")
    jc = lax.axis_index("col")
    j = lax.div(jc, CORES)
    c = lax.rem(jc, CORES)
    n_col = RING * CORES

    def wrap(v):
        return lax.rem(v + RING, RING)

    p = wrap(j - i)
    diag_chip = p == 0
    left, right = wrap(j + 3), wrap(j + 1)
    up, down = wrap(i + 3), wrap(i + 1)
    opp, iopp = wrap(j + 2), wrap(i + 2)
    partner = {"col": j * CORES + (1 - c)}
    to_x = ({"col": right * CORES + c}, {"col": left * CORES + c})
    to_y = ({"row": down}, {"row": up})
    half_cols = pl.ds(pl.multiple_of(c * rb, rb), rb)

    def copy(src, dst, send, recv, dev):
        return pltpu.make_async_remote_copy(
            src_ref=src, dst_ref=dst, send_sem=send, recv_sem=recv, device_id=dev, device_id_type=MESH
        )

    def send(ref, ss, rs, dev):
        copy(ref, ref, ss, rs, dev).start()

    def wait_recv(ref, rs):
        copy(ref, ref, d_send.at[0], rs, partner).wait_recv()

    def wait_send(ref, ss):
        copy(ref, ref, ss, d_recv.at[0, 0], partner).wait_send()

    def red_put(idx, vals):
        sub = lax.broadcasted_iota(jnp.int32, (8, 128), 0)
        tile = jnp.zeros((8, 128), jnp.float32)
        for r, v in enumerate(vals):
            tile = jnp.where(sub == r, v, tile)
        red_a[idx, jc] = tile

    def red_send(idx):
        for k in range(1, n_col):
            dev = lax.rem(jc + k, n_col)
            send(red_a.at[idx, jc], a_send.at[idx], a_recv.at[idx], {"col": dev})

    def red_mid_put(idx):
        wait_recv(red_a.at[idx, pl.ds(0, n_col - 1)], a_recv.at[idx])
        red_b[idx, i] = jnp.sum(red_a[idx], axis=0)

    def red_mid_send(idx):
        for k in range(1, RING):
            send(red_b.at[idx, i], b_send.at[idx], b_recv.at[idx], {"row": wrap(i + k)})

    def red_get(idx):
        wait_recv(red_b.at[idx, pl.ds(0, RING - 1)], b_recv.at[idx])
        wait_send(red_a.at[idx, pl.ds(0, n_col - 1)], a_send.at[idx])
        wait_send(red_b.at[idx, pl.ds(0, RING - 1)], b_send.at[idx])
        total = jnp.sum(red_b[idx], axis=0)
        return [total[r : r + 1, 0:1] for r in range(3)]

    def total_of(v):
        return jnp.sum(v, axis=1, keepdims=True)

    def is_diag(m):
        row_id = lax.broadcasted_iota(jnp.int32, (pr, cb), 0) + (m * pr + c * rb + (j - i) * cb)
        return row_id == lax.broadcasted_iota(jnp.int32, (pr, cb), 1)

    def piece_rows(m):
        return pl.ds(pl.multiple_of(lax.rem(m, per) * pr, pr), pr)

    def put_x(m, val, buf):
        cols[j, lax.div(m, per), c, piece_rows(m)] = val
        for q in range(PARTS):
            for h in range(CORES):
                at = h * rb + q * qr
                rows[buf, i, q, h, pl.ds(pl.multiple_of(m * pr, pr), pr)] = val[:, at : at + qr]

    barrier = pltpu.get_barrier_semaphore()
    for k in range(1, n_col):
        pl.semaphore_signal(barrier, inc=1, device_id={"col": lax.rem(jc + k, n_col)}, device_id_type=MESH)
    for k in range(1, RING):
        pl.semaphore_signal(barrier, inc=1, device_id={"row": wrap(i + k)}, device_id_type=MESH)
    for t in range(cb // qr):
        ham_t[:, t * qr : (t + 1) * qr] = ham[t * qr : (t + 1) * qr, :].T

    def trace_body(m, tr):
        blk = ham_t[pl.ds(pl.multiple_of(m * pr, pr), pr)]
        return tr + jnp.sum(jnp.where(is_diag(m), blk, 0.0), axis=0, keepdims=True)

    tr = lax.fori_loop(0, PIECES, trace_body, jnp.zeros((1, cb), jnp.float32))
    red_put(0, [total_of(tr)])
    pl.semaphore_wait(barrier, n_col + RING - 2)
    red_send(0)
    red_mid_put(0)
    red_mid_send(0)
    mu = red_get(0)[0] / order
    occ = jnp.full((1, 1), n_occ[0].astype(jnp.float32))
    eps_min = jnp.full((1, 1), bounds[0])
    eps_max = jnp.full((1, 1), bounds[1])
    lam = jnp.minimum(occ / (eps_max - mu), (order - occ) / (mu - eps_min)) / order

    @pl.loop(0, PIECES)
    def _(m):
        blk = ham_t[pl.ds(pl.multiple_of(m * pr, pr), pr)]
        put_x(m, jnp.where(is_diag(m), lam * (mu - blk) + occ / order, -lam * blk), 0)

    def step(s, carry):
        buf = lax.rem(s, 2)

        for q in range(PARTS):
            for o in range(2):
                for d in range(2):
                    h = d if o == 0 else 1 - d
                    send(cols.at[j, q, c, pl.ds(h * hr, hr)], x_send.at[d], x_recv.at[d, q, h], to_x[d])
                    send(rows.at[buf, i, q, h], y_send.at[d], y_recv.at[d, q, h], to_y[d])
            send(cols.at[j, q, c], d_send.at[0], d_recv.at[0, q], partner)
        acc[...] = jnp.zeros_like(acc)

        near = ((left, up), (right, down))

        def arrive_near(q):
            for d in range(2):
                kx, ky = near[d]
                xp = cols.at[kx, q, c, pl.ds(d * hr, hr)]
                wait_recv(xp, x_recv.at[d, q, d])
                send(xp, xf_send.at[d], xf_recv.at[d, q], to_x[d])
                yp = rows.at[buf, ky, q, d]
                wait_recv(yp, y_recv.at[d, q, d])
                send(yp, yf_send.at[d], yf_recv.at[d, q], to_y[d])
            for d in range(2):
                kx, ky = near[d]
                wait_recv(cols.at[kx, q, c, pl.ds((1 - d) * hr, hr)], x_recv.at[d, q, 1 - d])
                send(cols.at[kx, q, c], d_send.at[0], d_recv.at[3 if d == 0 else 1, q], partner)
                wait_recv(rows.at[buf, ky, q, 1 - d], y_recv.at[d, q, 1 - d])

        def arrive_far(q):
            for d in range(2):
                wait_recv(cols.at[opp, q, c, pl.ds(d * hr, hr)], xf_recv.at[d, q])
            send(cols.at[opp, q, c], d_send.at[0], d_recv.at[2, q], partner)
            for d in range(2):
                wait_recv(rows.at[buf, iopp, q, d], yf_recv.at[d, q])

        def item1(t, carry):
            in1 = t < jnp.where(diag_chip, 9, 6)
            late = jnp.maximum(t - 6, 0)
            q = jnp.where(
                in1,
                jnp.where(diag_chip, lax.div(t, 3), lax.div(t, 2)),
                jnp.where(diag_chip, jnp.maximum(t - 9, 0), lax.div(late, 2)),
            )
            u = jnp.where(
                in1,
                jnp.where(diag_chip, lax.rem(t, 3), lax.rem(t, 2)),
                jnp.where(diag_chip, 0, lax.rem(late, 2)),
            )
            k1 = jnp.where(
                diag_chip,
                i + jnp.where(u == 2, 3, u),
                jnp.where(p == 2, i + jnp.where(u == 0, 1, 3), jnp.where(u == 0, j, i)),
            )
            k = wrap(jnp.where(in1, k1, jnp.where(u == 0, i + 2, j + 2)))

            @pl.when(jnp.logical_and(in1, u == 0))
            def _():
                arrive_near(q)

            @pl.when(jnp.logical_and(jnp.logical_not(in1), u == 0))
            def _():
                arrive_far(q)

            wait_recv(cols.at[k, q, 1 - c], d_recv.at[wrap(k - j), q])
            rhs = cols[k, q].reshape(CORES * qr, cb)
            own = cols[k, q, :, :, half_cols].reshape(CORES * qr, rb)
            lhs = jnp.concatenate(
                [jnp.concatenate([rows[buf, k, q, h] for h in range(CORES)], axis=1), own.T], axis=0
            )
            acc[...] += jnp.dot(lhs, rhs, precision=HIGHEST, preferred_element_type=jnp.float32)
            return carry

        lax.fori_loop(0, RING * PARTS, item1, 0)
        for d in range(2):
            wait_send(cols.at[j, :, c], x_send.at[d])
            wait_send(cols.at[j, :, c, pl.ds(0, hr)], xf_send.at[d])
            wait_send(rows.at[buf, i], y_send.at[d])
            wait_send(rows.at[buf, i, :, 0], yf_send.at[d])
        wait_send(cols.at[:, :, c], d_send.at[0])

        for q in range(PARTS):
            sq[j, q, c] = acc[q * qr : (q + 1) * qr]

        @pl.when(jnp.logical_not(diag_chip))
        def _():
            for q in range(PARTS):
                sq[i, q, c] = acc[rb + q * qr : rb + (q + 1) * qr]

        k_left = jnp.where(p == 1, opp, left)
        k_right = jnp.where(p == 3, opp, right)

        def send_pieces(lo, hi):
            @pl.when(jnp.logical_not(diag_chip))
            def _():
                for m in range(lo, hi):
                    for d in range(2):
                        ref = sq.at[j, m // per, c, pl.ds((m % per) * pr, pr)]
                        send(ref, x2_send.at[d], x2_recv.at[d, m], to_x[d])

        send_pieces(0, per)
        def sums_body(m, carry):
            x = cols[j, lax.div(m, per), c, piece_rows(m)]
            x2 = acc[pl.ds(pl.multiple_of(m * pr, pr), pr)]
            t1 = jnp.sum(jnp.where(is_diag(m), x, 0.0), axis=0, keepdims=True)
            t2 = jnp.sum(x * x, axis=0, keepdims=True)
            t3 = jnp.sum(x2 * x, axis=0, keepdims=True)
            return carry[0] + t1, carry[1] + t2, carry[2] + t3

        zero = jnp.zeros((1, cb), jnp.float32)
        sums = lax.fori_loop(0, PIECES, sums_body, (zero, zero, zero))
        red_put(s + 1, [total_of(v) for v in sums])

        red_send(s + 1)
        send_pieces(per, PIECES)

        @pl.when(p == 2)
        def _():
            for q in range(PARTS):
                for h in range(CORES):
                    src = sq.at[j, :, c, :, pl.ds(h * rb + q * qr, qr)]
                    copy(src, tin.at[q, h], t_send.at[0], t_recv.at[q, h], {"row": j}).start()

        for q in range(PARTS):
            send(sq.at[j, q, c], d2_send.at[0], d2_recv.at[0, q], partner)

        @pl.when(jnp.logical_not(diag_chip))
        def _():
            for q in range(PARTS):
                send(sq.at[i, q, c], d2_send.at[0], d2_recv.at[3, q], partner)

        acc[0:rb] = jnp.zeros((rb, cb), jnp.float32)

        def arrive2(m):
            q = lax.div(m, per)
            u = lax.rem(m, per)
            for d, k in ((0, k_left), (1, k_right)):
                ref = sq.at[k, q, c, piece_rows(m)]
                wait_recv(ref, x2_recv.at[d, m])

                @pl.when(diag_chip)
                def _():
                    send(ref, x2_send.at[d], x2_recv.at[d, m], to_x[d])

            @pl.when(u == per - 1)
            def _():
                send(sq.at[k_left, q, c], d2_send.at[0], d2_recv.at[1, q], partner)
                send(sq.at[k_right, q, c], d2_send.at[0], d2_recv.at[2, q], partner)

            @pl.when(jnp.logical_and(diag_chip, u == per - 2))
            def _():
                for h in range(CORES):
                    wait_recv(tin.at[q, h], t_recv.at[q, h])
                    sq[opp, q, h, :, half_cols] = tin[q, h].reshape(rb, qr).T

            @pl.when(jnp.logical_and(diag_chip, u == per - 1))
            def _():
                ref = sq.at[opp, q, :, :, half_cols]
                send(ref, d2_send.at[0], d2_recv.at[3, q], partner)

        def item2(m, carry):
            @pl.when(m < PIECES)
            def _():
                arrive2(m)

            @pl.when(m == 6)
            def _():
                red_mid_put(s + 1)

            @pl.when(m == 7)
            def _():
                red_mid_send(s + 1)

            u = lax.rem(m, 4)
            qq = jnp.maximum(lax.div(m, 4) - 1, 0)
            early = m < 4
            kind = jnp.where(early, jnp.where(m < 3, 0, 3), u + 1)
            q = jnp.where(
                early, jnp.where(m < 3, m, 0), jnp.where(jnp.logical_and(u == 2, jnp.logical_not(diag_chip)), qq + 1, qq)
            )
            k = jnp.where(
                kind == 0, j, jnp.where(kind == 1, k_left, jnp.where(kind == 2, k_right, jnp.where(diag_chip, opp, i)))
            )
            work = jnp.where(
                early,
                jnp.logical_or(m < 3, jnp.logical_not(diag_chip)),
                jnp.logical_or(u < 2, jnp.logical_and(u == 2, jnp.logical_or(diag_chip, qq < 2))),
            )

            @pl.when(work)
            def _():
                @pl.when(jnp.logical_and(kind == 3, diag_chip))
                def _():
                    other = pl.ds(pl.multiple_of((1 - c) * rb, rb), rb)
                    wait_recv(sq.at[k, q, :, :, other], d2_recv.at[3, q])

                @pl.when(jnp.logical_not(jnp.logical_and(kind == 3, diag_chip)))
                def _():
                    wait_recv(sq.at[k, q, 1 - c], d2_recv.at[kind, q])

                lhs = jnp.concatenate([rows[buf, k, q, h] for h in range(CORES)], axis=1)
                rhs = sq[k, q].reshape(CORES * qr, cb)
                acc[0:rb] += jnp.dot(lhs, rhs, precision=HIGHEST, preferred_element_type=jnp.float32)

            return carry

        lax.fori_loop(0, PIECES + 3, item2, 0)
        for d in range(2):
            wait_send(sq.at[j, :, c], x2_send.at[d])
        wait_send(sq.at[:, :, c], d2_send.at[0])

        @pl.when(p == 2)
        def _():
            wait_send(sq.at[j, :, c], t_send.at[0])

        t1, t2, t3 = red_get(s + 1)
        mix = (t2 - t3) / (t1 - t2)
        a1 = (1.0 - 2.0 * mix) / (1.0 - mix)
        a2 = (1.0 + mix) / (1.0 - mix)
        a3 = 1.0 / (1.0 - mix)

        def update_body(m, carry):
            at = pl.ds(pl.multiple_of(m * pr, pr), pr)
            x = cols[j, lax.div(m, per), c, piece_rows(m)]
            x2 = sq[j, lax.div(m, per), c, piece_rows(m)]
            new = a1 * x + a2 * x2 - a3 * acc[at]
            put_x(m, new, lax.rem(s + 1, 2))
            return carry + jnp.sum(new * ham_t[at], axis=0, keepdims=True)

        en = lax.fori_loop(0, PIECES, update_body, zero)
        return total_of(en)

    en = lax.fori_loop(0, STEPS, step, jnp.zeros((1, 1), jnp.float32))
    last = STEPS + 1
    red_put(last, [en])
    for q in range(PARTS):
        out[:, q * qr : (q + 1) * qr] = cols[j, q, c].T
    red_send(last)
    red_mid_put(last)
    red_mid_send(last)
    energy[0] = jnp.sum(2.0 * red_get(last)[0])


def solution(mesh):
    def local_fn(ham_blk, bounds, n_occ):
        cb, rb = ham_blk.shape
        qr = rb // PARTS
        f32 = jnp.float32
        dma = pltpu.SemaphoreType.DMA
        vmem = pl.BlockSpec(memory_space=pltpu.VMEM)
        smem = pl.BlockSpec(memory_space=pltpu.SMEM)
        return pl.pallas_call(
            purify,
            out_shape=(jax.ShapeDtypeStruct((cb, rb), f32), jax.ShapeDtypeStruct((1,), f32)),
            in_specs=[vmem, smem, smem],
            out_specs=(vmem, smem),
            scratch_shapes=[
                pltpu.VMEM((RING, PARTS, CORES, qr, cb), f32),
                pltpu.VMEM((2, RING, PARTS, CORES, rb, qr), f32),
                pltpu.VMEM((RING, PARTS, CORES, qr, cb), f32),
                pltpu.VMEM((cb, cb), f32),
                pltpu.VMEM((PARTS, CORES, PARTS, qr, qr), f32),
                pltpu.VMEM((rb, cb), f32),
                pltpu.VMEM((STEPS + 2, RING * CORES, 8, 128), f32),
                pltpu.VMEM((STEPS + 2, RING, 8, 128), f32),
                dma((2, PARTS, 2)), dma((2, PARTS)), dma((2, PARTS, 2)), dma((2, PARTS)), dma((RING, PARTS)),
                dma((2,)), dma((2,)), dma((2,)), dma((2,)), dma((1,)),
                dma((2, PIECES)), dma((4, PARTS)), dma((PARTS, CORES)), dma((2,)), dma((1,)), dma((1,)),
                dma((STEPS + 2,)), dma((STEPS + 2,)), dma((STEPS + 2,)), dma((STEPS + 2,)),
            ],
            compiler_params=pltpu.CompilerParams(
                collective_id=0, has_side_effects=True, vmem_limit_bytes=56 * 2**20
            ),
        )(ham_blk, bounds, n_occ)

    spec_mat = P(("spin", "row"), "col")
    return jax.shard_map(
        local_fn, mesh=mesh, in_specs=(spec_mat, P("spin"), P("spin")), out_specs=(spec_mat, P("spin")), check_vma=False
    )
```

```python
import functools

import jax
import jax.numpy as jnp
from jax import lax
from jax.experimental import pallas as pl
from jax.experimental.pallas import tpu as pltpu
from jax.sharding import PartitionSpec as P

STEPS = 3
RING = 4
CORES = 2
PARTS = 3
PIECES = 12
MESH = pl.DeviceIdType.MESH
HIGHEST = lax.Precision.HIGHEST


def purify(
    ham, bounds, n_occ, out, energy,
    cols, rows, sq, acc, tin, ham_t, red_a, red_b,
    x_recv, xf_recv, y_recv, yf_recv, d_recv, x_send, xf_send, y_send, yf_send, d_send,
    x2_recv, d2_recv, t_recv, x2_send, d2_send, t_send, f_send, a_recv, a_send, b_recv, b_send,
):
    cb, rb = ham.shape
    qr = rb // PARTS
    hr = qr // 2
    pr = rb // PIECES
    order = cb * RING
    per = PIECES // PARTS
    i = lax.axis_index("row")
    jc = lax.axis_index("col")
    j = lax.div(jc, CORES)
    c = lax.rem(jc, CORES)
    n_col = RING * CORES

    def wrap(v):
        return lax.rem(v + RING, RING)

    p = wrap(j - i)
    diag_chip = p == 0
    left, right = wrap(j + 3), wrap(j + 1)
    up, down = wrap(i + 3), wrap(i + 1)
    opp, iopp = wrap(j + 2), wrap(i + 2)
    partner = {"col": j * CORES + (1 - c)}
    to_x = ({"col": right * CORES + c}, {"col": left * CORES + c})
    to_y = ({"row": down}, {"row": up})
    half_cols = pl.ds(pl.multiple_of(c * rb, rb), rb)

    def copy(src, dst, send, recv, dev):
        return pltpu.make_async_remote_copy(
            src_ref=src, dst_ref=dst, send_sem=send, recv_sem=recv, device_id=dev, device_id_type=MESH
        )

    def send(ref, ss, rs, dev):
        copy(ref, ref, ss, rs, dev).start()

    def wait_recv(ref, rs):
        copy(ref, ref, d_send.at[0], rs, partner).wait_recv()

    def wait_send(ref, ss):
        copy(ref, ref, ss, d_recv.at[0, 0], partner).wait_send()

    def red_put(idx, vals):
        sub = lax.broadcasted_iota(jnp.int32, (8, 128), 0)
        tile = jnp.zeros((8, 128), jnp.float32)
        for r, v in enumerate(vals):
            tile = jnp.where(sub == r, v, tile)
        red_a[idx, jc] = tile

    def red_send(idx):
        for k in range(1, n_col):
            dev = lax.rem(jc + k, n_col)
            send(red_a.at[idx, jc], a_send.at[idx], a_recv.at[idx], {"col": dev})

    def red_mid_put(idx):
        wait_recv(red_a.at[idx, pl.ds(0, n_col - 1)], a_recv.at[idx])
        red_b[idx, i] = jnp.sum(red_a[idx], axis=0)

    def red_mid_send(idx):
        for k in range(1, RING):
            send(red_b.at[idx, i], b_send.at[idx], b_recv.at[idx], {"row": wrap(i + k)})

    def red_get(idx):
        wait_recv(red_b.at[idx, pl.ds(0, RING - 1)], b_recv.at[idx])
        wait_send(red_a.at[idx, pl.ds(0, n_col - 1)], a_send.at[idx])
        wait_send(red_b.at[idx, pl.ds(0, RING - 1)], b_send.at[idx])
        total = jnp.sum(red_b[idx], axis=0)
        return [total[r : r + 1, 0:1] for r in range(3)]

    def total_of(v):
        return jnp.sum(v, axis=1, keepdims=True)

    def is_diag(m):
        row_id = lax.broadcasted_iota(jnp.int32, (pr, cb), 0) + (m * pr + c * rb + (j - i) * cb)
        return row_id == lax.broadcasted_iota(jnp.int32, (pr, cb), 1)

    def piece_rows(m):
        return pl.ds(pl.multiple_of(lax.rem(m, per) * pr, pr), pr)

    def put_x(m, val, buf):
        cols[j, lax.div(m, per), c, piece_rows(m)] = val
        for q in range(PARTS):
            for h in range(CORES):
                at = h * rb + q * qr
                rows[buf, i, q, h, pl.ds(pl.multiple_of(m * pr, pr), pr)] = val[:, at : at + qr]

    barrier = pltpu.get_barrier_semaphore()
    for k in range(1, n_col):
        pl.semaphore_signal(barrier, inc=1, device_id={"col": lax.rem(jc + k, n_col)}, device_id_type=MESH)
    for k in range(1, RING):
        pl.semaphore_signal(barrier, inc=1, device_id={"row": wrap(i + k)}, device_id_type=MESH)
    for t in range(cb // qr):
        ham_t[:, t * qr : (t + 1) * qr] = ham[t * qr : (t + 1) * qr, :].T

    def trace_body(m, tr):
        blk = ham_t[pl.ds(pl.multiple_of(m * pr, pr), pr)]
        return tr + jnp.sum(jnp.where(is_diag(m), blk, 0.0), axis=0, keepdims=True)

    tr = lax.fori_loop(0, PIECES, trace_body, jnp.zeros((1, cb), jnp.float32))
    red_put(0, [total_of(tr)])
    pl.semaphore_wait(barrier, n_col + RING - 2)
    red_send(0)
    red_mid_put(0)
    red_mid_send(0)
    mu = red_get(0)[0] / order
    occ = jnp.full((1, 1), n_occ[0].astype(jnp.float32))
    eps_min = jnp.full((1, 1), bounds[0])
    eps_max = jnp.full((1, 1), bounds[1])
    lam = jnp.minimum(occ / (eps_max - mu), (order - occ) / (mu - eps_min)) / order

    @pl.loop(0, PIECES)
    def _(m):
        blk = ham_t[pl.ds(pl.multiple_of(m * pr, pr), pr)]
        put_x(m, jnp.where(is_diag(m), lam * (mu - blk) + occ / order, -lam * blk), 0)

    def step(s, carry):
        buf = lax.rem(s, 2)

        for q in range(PARTS):
            for o in range(2):
                for d in range(2):
                    h = d if o == 0 else 1 - d
                    send(cols.at[j, q, c, pl.ds(h * hr, hr)], x_send.at[d], x_recv.at[d, q, h], to_x[d])
                    send(rows.at[buf, i, q, h], y_send.at[d], y_recv.at[d, q, h], to_y[d])
            send(cols.at[j, q, c], d_send.at[0], d_recv.at[0, q], partner)
        acc[...] = jnp.zeros_like(acc)

        near = ((left, up), (right, down))

        def arrive_near(q):
            for d in range(2):
                kx, ky = near[d]
                xp = cols.at[kx, q, c, pl.ds(d * hr, hr)]
                wait_recv(xp, x_recv.at[d, q, d])
                send(xp, xf_send.at[d], xf_recv.at[d, q], to_x[d])
                yp = rows.at[buf, ky, q, d]
                wait_recv(yp, y_recv.at[d, q, d])
                send(yp, yf_send.at[d], yf_recv.at[d, q], to_y[d])
            for d in range(2):
                kx, ky = near[d]
                wait_recv(cols.at[kx, q, c, pl.ds((1 - d) * hr, hr)], x_recv.at[d, q, 1 - d])
                send(cols.at[kx, q, c], d_send.at[0], d_recv.at[3 if d == 0 else 1, q], partner)
                wait_recv(rows.at[buf, ky, q, 1 - d], y_recv.at[d, q, 1 - d])

        def arrive_far(q):
            for d in range(2):
                wait_recv(cols.at[opp, q, c, pl.ds(d * hr, hr)], xf_recv.at[d, q])
            send(cols.at[opp, q, c], d_send.at[0], d_recv.at[2, q], partner)
            for d in range(2):
                wait_recv(rows.at[buf, iopp, q, d], yf_recv.at[d, q])

        def item1(t, carry):
            in1 = t < jnp.where(diag_chip, 9, 6)
            late = jnp.maximum(t - 6, 0)
            q = jnp.where(
                in1,
                jnp.where(diag_chip, lax.div(t, 3), lax.div(t, 2)),
                jnp.where(diag_chip, jnp.maximum(t - 9, 0), lax.div(late, 2)),
            )
            u = jnp.where(
                in1,
                jnp.where(diag_chip, lax.rem(t, 3), lax.rem(t, 2)),
                jnp.where(diag_chip, 0, lax.rem(late, 2)),
            )
            k1 = jnp.where(
                diag_chip,
                i + jnp.where(u == 2, 3, u),
                jnp.where(p == 2, i + jnp.where(u == 0, 1, 3), jnp.where(u == 0, j, i)),
            )
            k = wrap(jnp.where(in1, k1, jnp.where(u == 0, i + 2, j + 2)))

            @pl.when(jnp.logical_and(in1, u == 0))
            def _():
                arrive_near(q)

            @pl.when(jnp.logical_and(jnp.logical_not(in1), u == 0))
            def _():
                arrive_far(q)

            wait_recv(cols.at[k, q, 1 - c], d_recv.at[wrap(k - j), q])
            rhs = cols[k, q].reshape(CORES * qr, cb)
            own = cols[k, q, :, :, half_cols].reshape(CORES * qr, rb)
            lhs = jnp.concatenate(
                [jnp.concatenate([rows[buf, k, q, h] for h in range(CORES)], axis=1), own.T], axis=0
            )
            acc[...] += jnp.dot(lhs, rhs, precision=HIGHEST, preferred_element_type=jnp.float32)
            return carry

        lax.fori_loop(0, RING * PARTS, item1, 0)
        for d in range(2):
            wait_send(cols.at[j, :, c], x_send.at[d])
            wait_send(cols.at[j, :, c, pl.ds(0, hr)], xf_send.at[d])
            wait_send(rows.at[buf, i], y_send.at[d])
            wait_send(rows.at[buf, i, :, 0], yf_send.at[d])
        wait_send(cols.at[:, :, c], d_send.at[0])

        for q in range(PARTS):
            sq[j, q, c] = acc[q * qr : (q + 1) * qr]

        @pl.when(jnp.logical_not(diag_chip))
        def _():
            for q in range(PARTS):
                sq[i, q, c] = acc[rb + q * qr : rb + (q + 1) * qr]

        k_left = jnp.where(p == 1, opp, left)
        k_right = jnp.where(p == 3, opp, right)
        d_first = jnp.where(p == 1, 1, 0)
        k_first = jnp.where(p == 1, k_right, k_left)
        k_second = jnp.where(p == 1, k_left, k_right)

        def send_pieces(lo, hi):
            @pl.when(jnp.logical_not(diag_chip))
            def _():
                for n in range(lo, hi):
                    for d in range(2):
                        m = jnp.where(p == (1 if d == 0 else 3), (n + PIECES - 1) % PIECES, n)
                        ref = sq.at[j, lax.div(m, per), c, piece_rows(m)]
                        send(ref, x2_send.at[d], x2_recv.at[d, m], to_x[d])

        send_pieces(0, per)
        def sums_body(m, carry):
            x = cols[j, lax.div(m, per), c, piece_rows(m)]
            x2 = acc[pl.ds(pl.multiple_of(m * pr, pr), pr)]
            t1 = jnp.sum(jnp.where(is_diag(m), x, 0.0), axis=0, keepdims=True)
            t2 = jnp.sum(x * x, axis=0, keepdims=True)
            t3 = jnp.sum(x2 * x, axis=0, keepdims=True)
            return carry[0] + t1, carry[1] + t2, carry[2] + t3

        zero = jnp.zeros((1, cb), jnp.float32)
        sums = lax.fori_loop(0, PIECES, sums_body, (zero, zero, zero))
        red_put(s + 1, [total_of(v) for v in sums])

        red_send(s + 1)
        send_pieces(per, PIECES)

        @pl.when(p == 2)
        def _():
            for q in range(PARTS):
                for h in range(CORES):
                    src = sq.at[j, :, c, :, pl.ds(h * rb + q * qr, qr)]
                    copy(src, tin.at[q, h], t_send.at[0], t_recv.at[q, h], {"row": j}).start()

        for q in range(PARTS):
            send(sq.at[j, q, c], d2_send.at[0], d2_recv.at[0, q], partner)

        @pl.when(jnp.logical_not(diag_chip))
        def _():
            for q in range(PARTS):
                send(sq.at[i, q, c], d2_send.at[0], d2_recv.at[3, q], partner)

        acc[0:rb] = jnp.zeros((rb, cb), jnp.float32)

        def arrive2(m):
            q = lax.div(m, per)
            u = lax.rem(m, per)

            @pl.when(jnp.logical_and(p == 2, m == 0))
            def _():
                for d, k in ((0, k_left), (1, k_right)):
                    ref = sq.at[k, PARTS - 1, c, pl.ds((per - 1) * pr, pr)]
                    wait_recv(ref, x2_recv.at[d, PIECES - 1])
                    send(ref, f_send.at[d], x2_recv.at[1 - d, PIECES - 1], to_x[d])

            for n, k in enumerate((k_first, k_second)):
                d = d_first if n == 0 else 1 - d_first
                ref = sq.at[k, q, c, piece_rows(m)]

                @pl.when(jnp.logical_or(p != 2, m < PIECES - 1))
                def _():
                    wait_recv(ref, x2_recv.at[d, m])

                @pl.when(jnp.logical_and(diag_chip, m < PIECES - 1))
                def _():
                    send(ref, x2_send.at[n], x2_recv.at[n, m], to_x[n])

                @pl.when(u == per - 1)
                def _():
                    send(sq.at[k, q, c], d2_send.at[0], d2_recv.at[1 + n, q], partner)

            @pl.when(jnp.logical_and(diag_chip, u == per - 2))
            def _():
                for h in range(CORES):
                    wait_recv(tin.at[q, h], t_recv.at[q, h])
                    sq[opp, q, h, :, half_cols] = tin[q, h].reshape(rb, qr).T

            @pl.when(jnp.logical_and(diag_chip, u == per - 1))
            def _():
                ref = sq.at[opp, q, :, :, half_cols]
                send(ref, d2_send.at[0], d2_recv.at[3, q], partner)

        def item2(m, carry):
            @pl.when(m < PIECES)
            def _():
                arrive2(m)

            @pl.when(m == 6)
            def _():
                red_mid_put(s + 1)

            @pl.when(m == 7)
            def _():
                red_mid_send(s + 1)

            u = lax.rem(m, 4)
            qq = jnp.maximum(lax.div(m, 4) - 1, 0)
            early = m < 4
            kind = jnp.where(early, jnp.where(m < 3, 0, 3), u + 1)
            q = jnp.where(
                early, jnp.where(m < 3, m, 0), jnp.where(jnp.logical_and(u == 2, jnp.logical_not(diag_chip)), qq + 1, qq)
            )
            k = jnp.where(
                kind == 0, j, jnp.where(kind == 1, k_first, jnp.where(kind == 2, k_second, jnp.where(diag_chip, opp, i)))
            )
            work = jnp.where(
                early,
                jnp.logical_or(m < 3, jnp.logical_not(diag_chip)),
                jnp.logical_or(u < 2, jnp.logical_and(u == 2, jnp.logical_or(diag_chip, qq < 2))),
            )

            @pl.when(work)
            def _():
                @pl.when(jnp.logical_and(kind == 3, diag_chip))
                def _():
                    other = pl.ds(pl.multiple_of((1 - c) * rb, rb), rb)
                    wait_recv(sq.at[k, q, :, :, other], d2_recv.at[3, q])

                @pl.when(jnp.logical_not(jnp.logical_and(kind == 3, diag_chip)))
                def _():
                    wait_recv(sq.at[k, q, 1 - c], d2_recv.at[kind, q])

                lhs = jnp.concatenate([rows[buf, k, q, h] for h in range(CORES)], axis=1)
                rhs = sq[k, q].reshape(CORES * qr, cb)
                acc[0:rb] += jnp.dot(lhs, rhs, precision=HIGHEST, preferred_element_type=jnp.float32)

            return carry

        lax.fori_loop(0, PIECES + 3, item2, 0)

        @pl.when(diag_chip)
        def _():
            for d in range(2):
                wait_send(acc.at[pl.ds(0, (PIECES - 1) * pr)], x2_send.at[d])

        @pl.when(jnp.logical_not(diag_chip))
        def _():
            for d in range(2):
                wait_send(sq.at[j, :, c], x2_send.at[d])

        wait_send(sq.at[:, :, c], d2_send.at[0])

        @pl.when(p == 2)
        def _():
            wait_send(sq.at[j, :, c], t_send.at[0])
            for d in range(2):
                wait_send(sq.at[j, 0, c, pl.ds(0, pr)], f_send.at[d])

        t1, t2, t3 = red_get(s + 1)
        mix = (t2 - t3) / (t1 - t2)
        a1 = (1.0 - 2.0 * mix) / (1.0 - mix)
        a2 = (1.0 + mix) / (1.0 - mix)
        a3 = 1.0 / (1.0 - mix)

        def update_body(m, carry):
            at = pl.ds(pl.multiple_of(m * pr, pr), pr)
            x = cols[j, lax.div(m, per), c, piece_rows(m)]
            x2 = sq[j, lax.div(m, per), c, piece_rows(m)]
            new = a1 * x + a2 * x2 - a3 * acc[at]
            put_x(m, new, lax.rem(s + 1, 2))
            return carry + jnp.sum(new * ham_t[at], axis=0, keepdims=True)

        en = lax.fori_loop(0, PIECES, update_body, zero)
        return total_of(en)

    en = lax.fori_loop(0, STEPS, step, jnp.zeros((1, 1), jnp.float32))
    last = STEPS + 1
    red_put(last, [en])
    red_send(last)
    for q in range(PARTS):
        out[:, q * qr : (q + 1) * qr] = cols[j, q, c].T
    red_mid_put(last)
    red_mid_send(last)
    energy[0] = jnp.sum(2.0 * red_get(last)[0])


def solution(mesh):
    def local_fn(ham_blk, bounds, n_occ):
        cb, rb = ham_blk.shape
        qr = rb // PARTS
        f32 = jnp.float32
        dma = pltpu.SemaphoreType.DMA
        vmem = pl.BlockSpec(memory_space=pltpu.VMEM)
        smem = pl.BlockSpec(memory_space=pltpu.SMEM)
        return pl.pallas_call(
            purify,
            out_shape=(jax.ShapeDtypeStruct((cb, rb), f32), jax.ShapeDtypeStruct((1,), f32)),
            in_specs=[vmem, smem, smem],
            out_specs=(vmem, smem),
            scratch_shapes=[
                pltpu.VMEM((RING, PARTS, CORES, qr, cb), f32),
                pltpu.VMEM((2, RING, PARTS, CORES, rb, qr), f32),
                pltpu.VMEM((RING, PARTS, CORES, qr, cb), f32),
                pltpu.VMEM((cb, cb), f32),
                pltpu.VMEM((PARTS, CORES, PARTS, qr, qr), f32),
                pltpu.VMEM((rb, cb), f32),
                pltpu.VMEM((STEPS + 2, RING * CORES, 8, 128), f32),
                pltpu.VMEM((STEPS + 2, RING, 8, 128), f32),
                dma((2, PARTS, 2)), dma((2, PARTS)), dma((2, PARTS, 2)), dma((2, PARTS)), dma((RING, PARTS)),
                dma((2,)), dma((2,)), dma((2,)), dma((2,)), dma((1,)),
                dma((2, PIECES)), dma((4, PARTS)), dma((PARTS, CORES)), dma((2,)), dma((1,)), dma((1,)), dma((2,)),
                dma((STEPS + 2,)), dma((STEPS + 2,)), dma((STEPS + 2,)), dma((STEPS + 2,)),
            ],
            compiler_params=pltpu.CompilerParams(
                collective_id=0, has_side_effects=True, vmem_limit_bytes=56 * 2**20
            ),
        )(ham_blk, bounds, n_occ)

    spec_mat = P(("spin", "row"), "col")
    return jax.shard_map(
        local_fn, mesh=mesh, in_specs=(spec_mat, P("spin"), P("spin")), out_specs=(spec_mat, P("spin")), check_vma=False
    )
```

```python
import functools

import jax
import jax.numpy as jnp
from jax import lax
from jax.experimental import pallas as pl
from jax.experimental.pallas import tpu as pltpu
from jax.sharding import PartitionSpec as P

STEPS = 3
RING = 4
CORES = 2
PARTS = 3
PIECES = 12
MESH = pl.DeviceIdType.MESH
HIGHEST = lax.Precision.HIGHEST


def purify(
    ham, bounds, n_occ, out, energy,
    cols, rows, sq, acc, tin, ham_t, red_a, red_b, red_c,
    x_recv, xf_recv, y_recv, yf_recv, d_recv, x_send, xf_send, y_send, yf_send, d_send,
    x2_recv, d2_recv, t_recv, x2_send, d2_send, t_send, f_send, a_recv, a_send, b_recv, b_send, c_recv, c_send,
):
    cb, rb = ham.shape
    qr = rb // PARTS
    hr = qr // 2
    pr = rb // PIECES
    order = cb * RING
    per = PIECES // PARTS
    i = lax.axis_index("row")
    jc = lax.axis_index("col")
    j = lax.div(jc, CORES)
    c = lax.rem(jc, CORES)
    n_col = RING * CORES

    def wrap(v):
        return lax.rem(v + RING, RING)

    p = wrap(j - i)
    diag_chip = p == 0
    left, right = wrap(j + 3), wrap(j + 1)
    up, down = wrap(i + 3), wrap(i + 1)
    opp, iopp = wrap(j + 2), wrap(i + 2)
    partner = {"col": j * CORES + (1 - c)}
    to_x = ({"col": right * CORES + c}, {"col": left * CORES + c})
    to_y = ({"row": down}, {"row": up})
    half_cols = pl.ds(pl.multiple_of(c * rb, rb), rb)

    def copy(src, dst, send, recv, dev):
        return pltpu.make_async_remote_copy(
            src_ref=src, dst_ref=dst, send_sem=send, recv_sem=recv, device_id=dev, device_id_type=MESH
        )

    def send(ref, ss, rs, dev):
        copy(ref, ref, ss, rs, dev).start()

    def wait_recv(ref, rs):
        copy(ref, ref, d_send.at[0], rs, partner).wait_recv()

    def wait_send(ref, ss):
        copy(ref, ref, ss, d_recv.at[0, 0], partner).wait_send()

    def red_put(idx, vals):
        sub = lax.broadcasted_iota(jnp.int32, (8, 128), 0)
        tile = jnp.zeros((8, 128), jnp.float32)
        for r, v in enumerate(vals):
            tile = jnp.where(sub == r, v, tile)
        red_a[idx, jc] = tile

    def red_send(idx):
        for k in range(1, n_col):
            dev = lax.rem(jc + k, n_col)
            send(red_a.at[idx, jc], a_send.at[idx], a_recv.at[idx], {"col": dev})

    def red_mid_put(idx):
        wait_recv(red_a.at[idx, pl.ds(0, n_col - 1)], a_recv.at[idx])
        red_b[idx, i] = jnp.sum(red_a[idx], axis=0)

    def red_mid_send(idx):
        for k in range(1, RING):
            send(red_b.at[idx, i], b_send.at[idx], b_recv.at[idx], {"row": wrap(i + k)})

    def red_get(idx):
        wait_recv(red_b.at[idx, pl.ds(0, RING - 1)], b_recv.at[idx])
        wait_send(red_a.at[idx, pl.ds(0, n_col - 1)], a_send.at[idx])
        wait_send(red_b.at[idx, pl.ds(0, RING - 1)], b_send.at[idx])
        total = jnp.sum(red_b[idx], axis=0)
        return [total[r : r + 1, 0:1] for r in range(3)]

    def total_of(v):
        return jnp.sum(v, axis=1, keepdims=True)

    def is_diag(m):
        row_id = lax.broadcasted_iota(jnp.int32, (pr, cb), 0) + (m * pr + c * rb + (j - i) * cb)
        return row_id == lax.broadcasted_iota(jnp.int32, (pr, cb), 1)

    def piece_rows(m):
        return pl.ds(pl.multiple_of(lax.rem(m, per) * pr, pr), pr)

    def put_x(m, val, buf):
        cols[j, lax.div(m, per), c, piece_rows(m)] = val
        for q in range(PARTS):
            for h in range(CORES):
                at = h * rb + q * qr
                rows[buf, i, q, h, pl.ds(pl.multiple_of(m * pr, pr), pr)] = val[:, at : at + qr]

    others = [
        {"row": wrap(i + a), "col": lax.rem(jc + b, n_col)} for a in range(RING) for b in range(n_col) if a or b
    ]
    me = i * n_col + jc

    def all_put(idx, v):
        red_c[idx, me] = jnp.zeros((8, 128), jnp.float32) + v

    def all_send(idx):
        for dev in others:
            send(red_c.at[idx, me], c_send.at[idx], c_recv.at[idx], dev)

    def all_get(idx):
        wait_recv(red_c.at[idx, pl.ds(0, len(others))], c_recv.at[idx])
        wait_send(red_c.at[idx, pl.ds(0, len(others))], c_send.at[idx])
        return jnp.sum(red_c[idx], axis=0)[0:1, 0:1]

    def send_x(buf):
        for q in range(PARTS):
            for o in range(2):
                for d in range(2):
                    h = d if o == 0 else 1 - d
                    send(cols.at[j, q, c, pl.ds(h * hr, hr)], x_send.at[d], x_recv.at[d, q, h], to_x[d])
                    send(rows.at[buf, i, q, h], y_send.at[d], y_recv.at[d, q, h], to_y[d])
            send(cols.at[j, q, c], d_send.at[0], d_recv.at[0, q], partner)

    barrier = pltpu.get_barrier_semaphore()
    for dev in others:
        pl.semaphore_signal(barrier, inc=1, device_id=dev, device_id_type=MESH)
    for t in range(cb // qr):
        ham_t[:, t * qr : (t + 1) * qr] = ham[t * qr : (t + 1) * qr, :].T

    def trace_body(m, tr):
        blk = ham_t[pl.ds(pl.multiple_of(m * pr, pr), pr)]
        return tr + jnp.sum(jnp.where(is_diag(m), blk, 0.0), axis=0, keepdims=True)

    tr = lax.fori_loop(0, PIECES, trace_body, jnp.zeros((1, cb), jnp.float32))
    all_put(0, total_of(tr))

    @pl.loop(0, PIECES)
    def _(m):
        put_x(m, ham_t[pl.ds(pl.multiple_of(m * pr, pr), pr)], 0)

    pl.semaphore_wait(barrier, len(others))
    all_send(0)
    send_x(0)
    mu = all_get(0) / order
    occ = jnp.full((1, 1), n_occ[0].astype(jnp.float32))
    eps_min = jnp.full((1, 1), bounds[0])
    eps_max = jnp.full((1, 1), bounds[1])
    lam = jnp.minimum(occ / (eps_max - mu), (order - occ) / (mu - eps_min)) / order

    def to_density(v, row0, col0):
        on = lax.broadcasted_iota(jnp.int32, v.shape, 0) + (row0 - col0) == lax.broadcasted_iota(jnp.int32, v.shape, 1)
        return jnp.where(on, lam * (mu - v) + occ / order, -lam * v)

    def step(s, carry):
        buf = lax.rem(s, 2)

        acc[...] = jnp.zeros_like(acc)

        near = ((left, up), (right, down))

        def arrive_near(q):
            for d in range(2):
                kx, ky = near[d]
                xp = cols.at[kx, q, c, pl.ds(d * hr, hr)]
                wait_recv(xp, x_recv.at[d, q, d])
                send(xp, xf_send.at[d], xf_recv.at[d, q], to_x[d])
                yp = rows.at[buf, ky, q, d]
                wait_recv(yp, y_recv.at[d, q, d])
                send(yp, yf_send.at[d], yf_recv.at[d, q], to_y[d])
            for d in range(2):
                kx, ky = near[d]
                wait_recv(cols.at[kx, q, c, pl.ds((1 - d) * hr, hr)], x_recv.at[d, q, 1 - d])
                send(cols.at[kx, q, c], d_send.at[0], d_recv.at[3 if d == 0 else 1, q], partner)
                wait_recv(rows.at[buf, ky, q, 1 - d], y_recv.at[d, q, 1 - d])

        def arrive_far(q):
            for d in range(2):
                wait_recv(cols.at[opp, q, c, pl.ds(d * hr, hr)], xf_recv.at[d, q])
            send(cols.at[opp, q, c], d_send.at[0], d_recv.at[2, q], partner)
            for d in range(2):
                wait_recv(rows.at[buf, iopp, q, d], yf_recv.at[d, q])

        def item1(t, carry):
            in1 = t < jnp.where(diag_chip, 9, 6)
            late = jnp.maximum(t - 6, 0)
            q = jnp.where(
                in1,
                jnp.where(diag_chip, lax.div(t, 3), lax.div(t, 2)),
                jnp.where(diag_chip, jnp.maximum(t - 9, 0), lax.div(late, 2)),
            )
            u = jnp.where(
                in1,
                jnp.where(diag_chip, lax.rem(t, 3), lax.rem(t, 2)),
                jnp.where(diag_chip, 0, lax.rem(late, 2)),
            )
            k1 = jnp.where(
                diag_chip,
                i + jnp.where(u == 2, 3, u),
                jnp.where(p == 2, i + jnp.where(u == 0, 1, 3), jnp.where(u == 0, j, i)),
            )
            k = wrap(jnp.where(in1, k1, jnp.where(u == 0, i + 2, j + 2)))

            @pl.when(jnp.logical_and(in1, u == 0))
            def _():
                arrive_near(q)

            @pl.when(jnp.logical_and(jnp.logical_not(in1), u == 0))
            def _():
                arrive_far(q)

            wait_recv(cols.at[k, q, 1 - c], d_recv.at[wrap(k - j), q])

            def product(tile):
                row0 = k * cb + q * qr
                rhs = [tile(cols[k, q, h], row0 + h * rb, i * cb) for h in range(CORES)]
                own = [tile(cols[k, q, h, :, half_cols], row0 + h * rb, i * cb + c * rb) for h in range(CORES)]
                top = [tile(rows[buf, k, q, h], j * cb + c * rb, row0 + h * rb) for h in range(CORES)]
                lhs = jnp.concatenate(
                    [jnp.concatenate(top, axis=1), jnp.concatenate(own, axis=0).T], axis=0
                )
                acc[...] += jnp.dot(
                    lhs, jnp.concatenate(rhs, axis=0), precision=HIGHEST, preferred_element_type=jnp.float32
                )

            @pl.when(s == 0)
            def _():
                product(to_density)

            @pl.when(s > 0)
            def _():
                product(lambda v, row0, col0: v)

            return carry

        lax.fori_loop(0, RING * PARTS, item1, 0)
        for d in range(2):
            wait_send(cols.at[j, :, c], x_send.at[d])
            wait_send(cols.at[j, :, c, pl.ds(0, hr)], xf_send.at[d])
            wait_send(rows.at[buf, i], y_send.at[d])
            wait_send(rows.at[buf, i, :, 0], yf_send.at[d])
        wait_send(cols.at[:, :, c], d_send.at[0])

        for q in range(PARTS):
            sq[j, q, c] = acc[q * qr : (q + 1) * qr]

        @pl.when(jnp.logical_not(diag_chip))
        def _():
            for q in range(PARTS):
                sq[i, q, c] = acc[rb + q * qr : rb + (q + 1) * qr]

        k_left = jnp.where(p == 1, opp, left)
        k_right = jnp.where(p == 3, opp, right)
        d_first = jnp.where(p == 1, 1, 0)
        k_first = jnp.where(p == 1, k_right, k_left)
        k_second = jnp.where(p == 1, k_left, k_right)

        def send_pieces(lo, hi):
            @pl.when(jnp.logical_not(diag_chip))
            def _():
                for n in range(lo, hi):
                    for d in range(2):
                        m = jnp.where(p == (1 if d == 0 else 3), (n + PIECES - 1) % PIECES, n)
                        ref = sq.at[j, lax.div(m, per), c, piece_rows(m)]
                        send(ref, x2_send.at[d], x2_recv.at[d, m], to_x[d])

        send_pieces(0, per)

        @pl.when(s == 0)
        def _():
            for q in range(PARTS):
                cols[j, q, c] = to_density(cols[j, q, c], j * cb + c * rb + q * qr, i * cb)

            @pl.loop(0, RING * PARTS)
            def _(t):
                k, q = lax.div(t, PARTS), lax.rem(t, PARTS)
                for h in range(CORES):
                    rows[buf, k, q, h] = to_density(
                        rows[buf, k, q, h], j * cb + c * rb, k * cb + h * rb + q * qr
                    )

        def sums_body(m, carry):
            x = cols[j, lax.div(m, per), c, piece_rows(m)]
            x2 = acc[pl.ds(pl.multiple_of(m * pr, pr), pr)]
            t1 = jnp.sum(jnp.where(is_diag(m), x, 0.0), axis=0, keepdims=True)
            t2 = jnp.sum(x * x, axis=0, keepdims=True)
            t3 = jnp.sum(x2 * x, axis=0, keepdims=True)
            return carry[0] + t1, carry[1] + t2, carry[2] + t3

        zero = jnp.zeros((1, cb), jnp.float32)
        sums = lax.fori_loop(0, PIECES, sums_body, (zero, zero, zero))
        red_put(s + 1, [total_of(v) for v in sums])

        red_send(s + 1)
        send_pieces(per, PIECES)

        @pl.when(p == 2)
        def _():
            for q in range(PARTS):
                for h in range(CORES):
                    src = sq.at[j, :, c, :, pl.ds(h * rb + q * qr, qr)]
                    copy(src, tin.at[q, h], t_send.at[0], t_recv.at[q, h], {"row": j}).start()

        for q in range(PARTS):
            send(sq.at[j, q, c], d2_send.at[0], d2_recv.at[0, q], partner)

        @pl.when(jnp.logical_not(diag_chip))
        def _():
            for q in range(PARTS):
                send(sq.at[i, q, c], d2_send.at[0], d2_recv.at[3, q], partner)

        acc[0:rb] = jnp.zeros((rb, cb), jnp.float32)

        def arrive2(m):
            q = lax.div(m, per)
            u = lax.rem(m, per)

            @pl.when(jnp.logical_and(p == 2, m == 0))
            def _():
                for d, k in ((0, k_left), (1, k_right)):
                    ref = sq.at[k, PARTS - 1, c, pl.ds((per - 1) * pr, pr)]
                    wait_recv(ref, x2_recv.at[d, PIECES - 1])
                    send(ref, f_send.at[d], x2_recv.at[1 - d, PIECES - 1], to_x[d])

            for n, k in enumerate((k_first, k_second)):
                d = d_first if n == 0 else 1 - d_first
                ref = sq.at[k, q, c, piece_rows(m)]

                @pl.when(jnp.logical_or(p != 2, m < PIECES - 1))
                def _():
                    wait_recv(ref, x2_recv.at[d, m])

                @pl.when(jnp.logical_and(diag_chip, m < PIECES - 1))
                def _():
                    send(ref, x2_send.at[n], x2_recv.at[n, m], to_x[n])

                @pl.when(u == per - 1)
                def _():
                    send(sq.at[k, q, c], d2_send.at[0], d2_recv.at[1 + n, q], partner)

        def arrive_turned(m):
            q = lax.div(m, per) - 1

            @pl.when(lax.rem(m, per) == 0)
            def _():
                for h in range(CORES):
                    wait_recv(tin.at[q, h], t_recv.at[q, h])
                    sq[opp, q, h, :, half_cols] = tin[q, h].reshape(rb, qr).T

            @pl.when(lax.rem(m, per) == 1)
            def _():
                send(sq.at[opp, q, :, :, half_cols], d2_send.at[0], d2_recv.at[3, q], partner)

        def item2(m, carry):
            @pl.when(m < PIECES)
            def _():
                arrive2(m)

            @pl.when(jnp.logical_and(diag_chip, m >= per))
            def _():
                arrive_turned(m)

            @pl.when(m == 6)
            def _():
                red_mid_put(s + 1)

            @pl.when(m == 7)
            def _():
                red_mid_send(s + 1)

            u = lax.rem(m, 4)
            qq = jnp.maximum(lax.div(m, 4) - 1, 0)
            early = m < 4
            kind = jnp.where(early, jnp.where(m < 3, 0, 3), u + 1)
            q = jnp.where(
                early, jnp.where(m < 3, m, 0), jnp.where(jnp.logical_and(u == 2, jnp.logical_not(diag_chip)), qq + 1, qq)
            )
            k = jnp.where(
                kind == 0, j, jnp.where(kind == 1, k_first, jnp.where(kind == 2, k_second, jnp.where(diag_chip, opp, i)))
            )
            work = jnp.where(
                early,
                jnp.logical_or(m < 3, jnp.logical_not(diag_chip)),
                jnp.logical_or(u < 2, jnp.logical_and(u == 2, jnp.logical_or(diag_chip, qq < 2))),
            )

            @pl.when(work)
            def _():
                @pl.when(jnp.logical_and(kind == 3, diag_chip))
                def _():
                    other = pl.ds(pl.multiple_of((1 - c) * rb, rb), rb)
                    wait_recv(sq.at[k, q, :, :, other], d2_recv.at[3, q])

                @pl.when(jnp.logical_not(jnp.logical_and(kind == 3, diag_chip)))
                def _():
                    wait_recv(sq.at[k, q, 1 - c], d2_recv.at[kind, q])

                lhs = jnp.concatenate([rows[buf, k, q, h] for h in range(CORES)], axis=1)
                rhs = sq[k, q].reshape(CORES * qr, cb)
                acc[0:rb] += jnp.dot(lhs, rhs, precision=HIGHEST, preferred_element_type=jnp.float32)

            return carry

        lax.fori_loop(0, PIECES + 3, item2, 0)

        @pl.when(diag_chip)
        def _():
            for d in range(2):
                wait_send(acc.at[pl.ds(0, (PIECES - 1) * pr)], x2_send.at[d])

        @pl.when(jnp.logical_not(diag_chip))
        def _():
            for d in range(2):
                wait_send(sq.at[j, :, c], x2_send.at[d])

        wait_send(sq.at[:, :, c], d2_send.at[0])

        @pl.when(p == 2)
        def _():
            wait_send(sq.at[j, :, c], t_send.at[0])
            for d in range(2):
                wait_send(sq.at[j, 0, c, pl.ds(0, pr)], f_send.at[d])

        t1, t2, t3 = red_get(s + 1)
        mix = (t2 - t3) / (t1 - t2)
        a1 = (1.0 - 2.0 * mix) / (1.0 - mix)
        a2 = (1.0 + mix) / (1.0 - mix)
        a3 = 1.0 / (1.0 - mix)

        def update_body(m, carry):
            at = pl.ds(pl.multiple_of(m * pr, pr), pr)
            x = cols[j, lax.div(m, per), c, piece_rows(m)]
            x2 = sq[j, lax.div(m, per), c, piece_rows(m)]
            new = a1 * x + a2 * x2 - a3 * acc[at]
            put_x(m, new, lax.rem(s + 1, 2))
            return carry + jnp.sum(new * ham_t[at], axis=0, keepdims=True)

        en = lax.fori_loop(0, PIECES, update_body, zero)

        @pl.when(s < STEPS - 1)
        def _():
            send_x(lax.rem(s + 1, 2))

        return total_of(en)

    en = lax.fori_loop(0, STEPS, step, jnp.zeros((1, 1), jnp.float32))
    all_put(1, en)
    all_send(1)
    for q in range(PARTS):
        out[:, q * qr : (q + 1) * qr] = cols[j, q, c].T
    energy[0] = jnp.sum(2.0 * all_get(1))


def solution(mesh):
    def local_fn(ham_blk, bounds, n_occ):
        cb, rb = ham_blk.shape
        qr = rb // PARTS
        f32 = jnp.float32
        dma = pltpu.SemaphoreType.DMA
        vmem = pl.BlockSpec(memory_space=pltpu.VMEM)
        smem = pl.BlockSpec(memory_space=pltpu.SMEM)
        return pl.pallas_call(
            purify,
            out_shape=(jax.ShapeDtypeStruct((cb, rb), f32), jax.ShapeDtypeStruct((1,), f32)),
            in_specs=[vmem, smem, smem],
            out_specs=(vmem, smem),
            scratch_shapes=[
                pltpu.VMEM((RING, PARTS, CORES, qr, cb), f32),
                pltpu.VMEM((2, RING, PARTS, CORES, rb, qr), f32),
                pltpu.VMEM((RING, PARTS, CORES, qr, cb), f32),
                pltpu.VMEM((cb, cb), f32),
                pltpu.VMEM((PARTS, CORES, PARTS, qr, qr), f32),
                pltpu.VMEM((rb, cb), f32),
                pltpu.VMEM((STEPS + 2, RING * CORES, 8, 128), f32),
                pltpu.VMEM((STEPS + 2, RING, 8, 128), f32),
                pltpu.VMEM((2, RING * RING * CORES, 8, 128), f32),
                dma((2, PARTS, 2)), dma((2, PARTS)), dma((2, PARTS, 2)), dma((2, PARTS)), dma((RING, PARTS)),
                dma((2,)), dma((2,)), dma((2,)), dma((2,)), dma((1,)),
                dma((2, PIECES)), dma((4, PARTS)), dma((PARTS, CORES)), dma((2,)), dma((1,)), dma((1,)), dma((2,)),
                dma((STEPS + 2,)), dma((STEPS + 2,)), dma((STEPS + 2,)), dma((STEPS + 2,)), dma((2,)), dma((2,)),
            ],
            compiler_params=pltpu.CompilerParams(
                collective_id=0, has_side_effects=True, vmem_limit_bytes=56 * 2**20
            ),
        )(ham_blk, bounds, n_occ)

    spec_mat = P(("spin", "row"), "col")
    return jax.shard_map(
        local_fn, mesh=mesh, in_specs=(spec_mat, P("spin"), P("spin")), out_specs=(spec_mat, P("spin")), check_vma=False
    )
```
